16 devices in a mesh: rows: 16 (over z, y, x, core).
Axes of the slice: x: 2, y: 2, z: 2, core: 2. Of those that a mesh axis runs over, the one named last changes fastest.
Arguments:
- a_mat: float32 [262144, 64], P('rows')
- b_mat: float32 [262144, 4], P('rows')
Outputs:
- output 1: float32 [262144, 64], P('rows')
- output 2: float32 [64, 64], replicated
- output 3: float32 [64, 4], replicated
All inputs are finite; a program needn't handle non-finite values.
Results may differ from the reference program's by a relative error of at most 0.001.
Values sent between devices are 32-bit elements.
A program may use at most 1 GiB of HBM per device.

```python
import jax
import jax.numpy as jnp

NUM_BLOCKS = 16
ROWS_DEV = 16384
COLS = 64
RHS = 4

TOTAL_ROWS = NUM_BLOCKS * ROWS_DEV


def setup_inputs(seed: int = 0) -> dict:
    key = jax.random.key(seed)
    key_gauss, key_weight, key_left, key_right, key_rhs = jax.random.split(key, 5)
    gauss = jax.random.normal(key_gauss, (NUM_BLOCKS, ROWS_DEV, COLS), jnp.float32)
    col_weight = jnp.exp(jax.random.normal(key_weight, (NUM_BLOCKS, 1, COLS), jnp.float32))
    col_weight = col_weight / jnp.sqrt(jnp.mean(col_weight * col_weight, axis=2, keepdims=True))
    left_rot = jnp.linalg.qr(jax.random.normal(key_left, (COLS, COLS), jnp.float32))[0]
    right_rot = jnp.linalg.qr(jax.random.normal(key_right, (COLS, COLS), jnp.float32))[0]
    spread = 10.0 ** jnp.linspace(0.0, -2.5, COLS, dtype=jnp.float32)
    spread = spread / jnp.sqrt(jnp.mean(spread * spread))
    mixing = jnp.dot(left_rot * spread[None, :], right_rot.T)
    weighted = (gauss * col_weight).reshape(TOTAL_ROWS, COLS)
    a_mat = jnp.dot(weighted, mixing) * (TOTAL_ROWS ** -0.5)
    b_mat = jax.random.normal(key_rhs, (TOTAL_ROWS, RHS), jnp.float32)
    return {'a_mat': a_mat, 'b_mat': b_mat}


def reference(a_mat, b_mat):
    q_raw, r_raw = jnp.linalg.qr(a_mat)
    diag_signs = jnp.sign(jnp.diagonal(r_raw))
    q_fac = q_raw * diag_signs[None, :]
    r_fac = r_raw * diag_signs[:, None]
    c_mat = jnp.dot(q_fac.T, b_mat, preferred_element_type=jnp.float32)
    return q_fac, r_fac, c_mat
```

```python
import jax
import jax.numpy as jnp
from jax import lax
from jax.experimental import pallas as pl
from jax.experimental.pallas import tpu as pltpu
from jax.sharding import PartitionSpec as P

HI = lax.Precision.HIGHEST
F32 = jnp.float32
N = 64
BLK = 8
SHIFT = 1e-6


def _row(v, k):
    return jnp.broadcast_to(v[k:k + 1, :], (BLK, 2 * N))


def _factor(w):
    w = list(w)
    sub = lax.broadcasted_iota(jnp.int32, (BLK, 2 * N), 0)
    out = []
    for p in range(N // BLK):
        cols = [[jnp.broadcast_to(blk[:, BLK * p + j:BLK * p + j + 1], (BLK, 2 * N)) for j in range(BLK)] for blk in w[p:]]
        row = w[p]
        mults, urows = [], []
        for k in range(BLK):
            inv = 1.0 / _row(cols[0][k], k)
            pivots = [_row(cols[0][j], k) for j in range(k + 1, BLK)]
            urow = _row(row, k)
            mult = [c[k] * inv for c in cols]
            mult[0] = jnp.where(sub > k, mult[0], 0.0)
            for i in range(len(cols)):
                for j in range(k + 1, BLK):
                    cols[i][j] = cols[i][j] - mult[i] * pivots[j - k - 1]
            row = row - mult[0] * urow
            mults.append(mult)
            urows.append(urow)
        for i in range(p + 1, N // BLK):
            for k in range(BLK):
                w[i] = w[i] - mults[k][i - p] * urows[k]
        diag = cols[0][0]
        for k in range(1, BLK):
            diag = jnp.where(sub == k, cols[0][k], diag)
        out.append(row * lax.rsqrt(diag))
    return out


def _factor_kernel(g_ref, o_ref):
    out = _factor([g_ref[BLK * i:BLK * i + BLK, :] for i in range(N // BLK)])
    for i in range(N // BLK):
        o_ref[BLK * i:BLK * i + BLK, :] = out[i]


def _cholesky(gram):
    both = pl.pallas_call(_factor_kernel, out_shape=jax.ShapeDtypeStruct((N, 2 * N), F32))(
        jnp.concatenate([gram, jnp.eye(N, dtype=F32)], axis=1))
    return jnp.triu(both[:, :N]), jnp.tril(both[:, N:])


def _dot(x, y, dims):
    return lax.dot_general(x, y, (dims, ((), ())), precision=HI, preferred_element_type=F32)


def solution(mesh):
    def local_fn(a_blk, b_blk):
        work = a_blk.T
        r_fac = None
        for step in range(3):
            gram = lax.psum(_dot(work, work, ((1,), (1,))), 'rows')
            if step == 0:
                gram = gram + (SHIFT * jnp.trace(gram)) * jnp.eye(N, dtype=F32)
            r_step, inv_t = _cholesky(gram)
            work = _dot(inv_t, work, ((1,), (0,)))
            r_fac = r_step if r_fac is None else _dot(r_step, r_fac, ((1,), (0,)))
        c_mat = lax.psum(_dot(work, b_blk.T, ((1,), (1,))), 'rows')
        return work.T, jnp.triu(r_fac), c_mat

    return jax.shard_map(local_fn, mesh=mesh, in_specs=(P('rows', None), P('rows', None)), out_specs=(P('rows', None), P(), P()), check_vma=False)
```

```python
import jax
import jax.numpy as jnp
from jax import lax
from jax.experimental import pallas as pl
from jax.experimental.pallas import tpu as pltpu
from jax.sharding import PartitionSpec as P


HI = lax.Precision.HIGHEST
F32 = jnp.float32
N = 64
RHS = 4
BLK = 8
LANES = 128
CHIPS = 8
PIECES = (2048, 4096, 5120, 5120)
SUB = 1024
AHEAD = 3
STORES = (2048,) * 7 + (1024,) * 2
HALF = N // 2
MSG = HALF + BLK
FAR_FIRST = (7, 6, 5, 3, 4, 2, 1)
NT, NN, TN = ((1,), (1,)), ((1,), (0,)), ((0,), (0,))
MESH = pl.DeviceIdType.MESH


def _dot(x, y, dims, precision=None):
    return lax.dot_general(x, y, (dims, ((), ())), precision=precision, preferred_element_type=F32)


def _two_sum(a, b):
    s = a + b
    t = s - a
    return s, (a - (s - t)) + (b - t)


def _scale(x, axis):
    q = jnp.max(jnp.abs(x), axis=axis, keepdims=True) * 8388609.0
    return jnp.abs(q - q * (1.0 - 2.0 ** -24))


def _slices(x, p):
    s1, s2, s3 = p * (1.5 * 2.0 ** 16), p * (1.5 * 2.0 ** 8), p * 1.5
    h1 = (x + s1) - s1
    r1 = x - h1
    h2 = (r1 + s2) - s2
    r2 = r1 - h2
    h3 = (r2 + s3) - s3
    return h1, h2, h3, r2 - h3


def _split3(x):
    c = x * 65537.0
    h1 = c - (c - x)
    r = x - h1
    c = r * 65537.0
    h2 = c - (c - r)
    return h1, h2, r - h2


def _gram_chunk(x, b, px, acc):
    s1, e1, g2, g3, gc = acc
    for q in range(x.shape[1] // SUB):
        h1, h2, h3, l = _slices(x[:, q * SUB:(q + 1) * SUB], px)
        c1, c2, c3 = _split3(b[:, q * SUB:(q + 1) * SUB])
        o = _dot(jnp.concatenate([h1, h2, h3, l], axis=0), jnp.concatenate([h1, h2, c1, c2, c3], axis=0), NT)
        s1, err = _two_sum(s1, o[:N, :2 * N])
        e1 = e1 + err
        g2 = g2 + o[N:2 * N, :2 * N]
        g3 = g3 + (o[2 * N:3 * N, :2 * N] + o[3 * N:, :2 * N])
        gc = gc + ((o[:N, 2 * N:] + o[N:2 * N, 2 * N:]) + (o[2 * N:3 * N, 2 * N:] + o[3 * N:, 2 * N:]))
    return s1, e1, g2, g3, gc


def _gram_finish(acc):
    s1, e1, g2, g3, gc = acc
    cross = s1[:, N:]
    small = e1[:, N:] + (g3[:, :N] + g3[:, N:])
    z, ez = _two_sum(cross, cross.T)
    h, ea = _two_sum(s1[:, :N], z)
    h, eb = _two_sum(h, g2[:, N:])
    lo = ((ea + eb) + ez) + e1[:, :N] + (small + small.T)
    hi, lo = _two_sum(h, lo)
    ct = gc.T
    ct = ct[:RHS] + (ct[RHS:2 * RHS] + ct[2 * RHS:])
    return hi, lo, ct


def _pack(hi, lo, bta):
    both = jnp.concatenate([hi, lo], axis=1)
    row = lax.broadcasted_iota(jnp.int32, (HALF, LANES), 0)
    col = lax.broadcasted_iota(jnp.int32, (HALF, LANES), 1) % N
    block = jnp.where(col - HALF > row, jnp.roll(both[:HALF], HALF, axis=1), both[HALF:])
    diag = jnp.sum(jnp.where(row == col, both[:HALF], 0.0), axis=0, keepdims=True)
    sub = lax.broadcasted_iota(jnp.int32, (BLK, LANES), 0)
    tail = jnp.concatenate([jnp.zeros((RHS, LANES), F32), jnp.concatenate([bta, jnp.zeros_like(bta)], axis=1)], axis=0)
    return jnp.concatenate([block, jnp.where(sub == 0, diag, tail)], axis=0)


def _unpack(block, diag):
    row = lax.broadcasted_iota(jnp.int32, (HALF, HALF), 0)
    col = lax.broadcasted_iota(jnp.int32, (HALF, HALF), 1)
    cross, tri = block[:, :HALF], block[:, HALF:]
    flip = tri.T
    first = jnp.where(row == col, diag[:, :HALF], jnp.where(col > row, tri, flip))
    last = jnp.where(col <= row, tri, flip)
    return jnp.concatenate([jnp.concatenate([first, cross.T], axis=1), jnp.concatenate([cross, last], axis=1)], axis=0)


def _fold(both, err):
    lane = lax.broadcasted_iota(jnp.int32, both.shape, 1)
    sub = lax.broadcasted_iota(jnp.int32, both.shape, 0)
    return both + jnp.where((lane >= N) & (sub <= HALF), jnp.roll(err, N, axis=1), 0.0)


def _row(v, k):
    return jnp.broadcast_to(v[k:k + 1, :], (BLK, LANES))


def _factor(g):
    row = lax.broadcasted_iota(jnp.int32, (N, N), 0)
    col = lax.broadcasted_iota(jnp.int32, (N, N), 1)
    full = jnp.concatenate([g, jnp.where(row == col, 1.0, 0.0)], axis=1)
    blocks = N // BLK
    w = [full[BLK * i:BLK * i + BLK] for i in range(blocks)]
    sub = lax.broadcasted_iota(jnp.int32, (BLK, LANES), 0)
    spread = lambda blk, p: [jnp.broadcast_to(blk[:, BLK * p + j:BLK * p + j + 1], (BLK, LANES)) for j in range(BLK)]
    diag = spread(w[0], 0)
    pivot = _row(diag[0], 0)
    out = []
    for p in range(blocks):
        below = [spread(blk, p) for blk in w[p + 1:]]
        ahead = spread(w[p + 1], p + 1) if p + 1 < blocks else None
        cur, pivots_done = w[p], pivot
        for k in range(BLK):
            inv = 1.0 / pivot
            if k > 0:
                pivots_done = jnp.where(sub == k, pivot, pivots_done)
            if k + 1 < BLK:
                link, pivot = _row(diag[k], k + 1), _row(diag[k + 1], k + 1)
                pivot = pivot - (link * link) * inv
            elif ahead is not None:
                link, pivot = _row(below[0][k], 0), _row(ahead[0], 0)
                pivot = pivot - (link * link) * inv
            tops = [_row(diag[j], k) for j in range(k + 1, BLK)]
            mult = jnp.where(sub > k, diag[k], 0.0) * inv
            urow = _row(cur, k)
            for j in range(k + 1, BLK):
                diag[j] = diag[j] - mult * tops[j - k - 1]
            cur = cur - mult * urow
            for i, cols in enumerate(below):
                scaled = cols[k] * inv
                for j in range(k + 1, BLK):
                    cols[j] = cols[j] - scaled * tops[j - k - 1]
                w[p + 1 + i] = w[p + 1 + i] - scaled * urow
                if i == 0:
                    ahead = [ahead[j] - scaled * _row(cols[k], j) for j in range(BLK)]
        out.append(cur * lax.rsqrt(pivots_done))
        diag = ahead
    out = jnp.concatenate(out, axis=0)
    return jnp.where(col >= row, out[:, :N], 0.0), jnp.where(col <= row, out[:, N:], 0.0)


def _exact_rest(first, o1, o2, o3, o4):
    blk = lambda o, i: o[N * i:N * i + N]
    t, e = _two_sum(first, -blk(o1, 0))
    t, ea = _two_sum(t, -blk(o1, 1))
    t, eb = _two_sum(t, -blk(o2, 0))
    t, ec = _two_sum(t, -blk(o2, 1))
    rest = (blk(o1, 2) + blk(o3, 0)) + (blk(o1, 3) + blk(o4, 0)) + ((blk(o2, 2) + blk(o3, 1)) + (blk(o2, 3) + blk(o4, 1)))
    rest = rest + ((blk(o3, 2) + blk(o4, 3)) + (blk(o3, 3) + blk(o4, 2)))
    return (t - rest) + ((e + ea) + (eb + ec))


def _refined(hi, lo):
    row = lax.broadcasted_iota(jnp.int32, (N, N), 0)
    col = lax.broadcasted_iota(jnp.int32, (N, N), 1)
    eye = jnp.where(row == col, 1.0, 0.0)
    r1, v = _factor(jnp.where(row == col, hi * (1.0 + 2.0 ** -19), hi))
    parts = _slices(r1, _scale(r1, 0))
    left = jnp.concatenate(parts, axis=1)
    f = _exact_rest(hi, *[_dot(left, part, TN) for part in parts]) + lo
    left = jnp.concatenate(_slices(v, _scale(v, 1)), axis=0)
    d = _exact_rest(eye, *[_dot(left, part, NT) for part in _slices(r1, _scale(r1, 1))])
    d = jnp.where(col <= row, d, 0.0)
    e = _dot(_dot(v, f, NN, HI), v, NT, HI) + (_dot(d, d, NT, HI) - (d + d.T))
    r2, v2 = _factor(eye + e)
    return r2, r1 + _dot(d, r1, TN, HI), v2, v


def _reduce_kernel(a_hbm, b_hbm, f_ref, bta_ref, a_buf, b_buf, slots, sums, a_sem, b_sem, send_sem, recv_sem, down_sem):
    me = lax.axis_index('rows')
    core = me % 2
    chip = me // 2
    partner = me + 1 - 2 * core
    steps = len(PIECES)
    edges = [sum(PIECES[:i]) for i in range(steps + 1)]
    copies = []
    for i in range(steps):
        win = pl.ds(edges[i], PIECES[i])
        copies.append(pltpu.make_async_copy(a_hbm.at[:, win], a_buf.at[:, win], a_sem.at[i]))
    b_copy = pltpu.make_async_copy(b_hbm, b_buf, b_sem)
    for copy in copies[:1] + [b_copy] + copies[1:AHEAD]:
        copy.start()
    barrier = pltpu.get_barrier_semaphore()
    x, y, z = chip % 2, (chip // 2) % 2, chip // 4
    flip = lambda bit, way: 1 - bit if way else bit
    peers = [8 * flip(z, far // 4) + 4 * flip(y, far // 2 % 2) + 2 * flip(x, far % 2) + core for far in FAR_FIRST]
    for peer in peers + [partner]:
        pl.semaphore_signal(barrier, inc=1, device_id=(peer,), device_id_type=MESH)

    zero = jnp.zeros((N, 2 * N), F32)
    acc = (zero, zero, zero, zero, jnp.zeros((N, 3 * RHS), F32))
    scale = None
    for i in range(steps + 1):
        nxt = None
        if i < steps:
            copies[i].wait()
            if i + AHEAD < steps:
                copies[i + AHEAD].start()
            nxt = _scale(a_buf[:, edges[i]:edges[i + 1]], 1)
        if i == 0:
            b_copy.wait()
        if i > 0:
            win = slice(edges[i - 1], edges[i])
            acc = _gram_chunk(a_buf[:, win], b_buf[:, win], scale, acc)
        scale = nxt
    hi, lo, bta = _gram_finish(acc)
    slots[pl.ds(chip, 1)] = _pack(hi, lo, bta)[None]
    pl.semaphore_wait(barrier, CHIPS)
    sends = [pltpu.make_async_remote_copy(
        src_ref=slots.at[chip], dst_ref=slots.at[chip], send_sem=send_sem.at[j], recv_sem=recv_sem.at[j],
        device_id=(peer,), device_id_type=MESH) for j, peer in enumerate(peers)]
    for send in sends:
        send.start()
    for send in sends:
        send.wait_recv()
    both, err = slots[0], jnp.zeros((MSG, LANES), F32)
    for j in range(1, CHIPS):
        both, e = _two_sum(both, slots[j])
        err = err + e
    sums[pl.ds(core, 1)] = _fold(both, err)[None]
    swap = pltpu.make_async_remote_copy(
        src_ref=sums.at[core], dst_ref=sums.at[core], send_sem=down_sem.at[0], recv_sem=down_sem.at[1],
        device_id=(partner,), device_id_type=MESH)
    swap.start()
    swap.wait_recv()
    got = _fold(*_two_sum(sums[0], sums[1]))
    r2, rc, v2, v = _refined(*[_unpack(got[:HALF, side:side + N], got[HALF:HALF + 1, side:side + N]) for side in (0, N)])
    f_ref[:, :LANES] = jnp.concatenate([r2, rc], axis=1)
    f_ref[:, LANES:] = jnp.concatenate([v2, v], axis=1)
    bta_ref[...] = got[HALF:, :]
    for send in sends:
        send.wait_send()
    swap.wait_send()


def _apply_kernel(f_ref, bta_ref, a_ref, q_hbm, r_hbm, c_hbm, q_buf, r_buf, c_buf, q_sem, small_sem):
    inv_t = _dot(f_ref[:, LANES:LANES + N], f_ref[:, LANES + N:], NN, HI)
    w = jnp.concatenate([jnp.concatenate([m] * 3, axis=1) for m in _split3(inv_t)], axis=0)
    copies = []
    start = 0
    for i, size in enumerate(STORES):
        win = pl.ds(start, size)
        o = _dot(w, jnp.concatenate(_split3(a_ref[:, win]), axis=0), NN)
        q_buf[:, win] = o[:N] + (o[N:2 * N] + o[2 * N:])
        copies.append(pltpu.make_async_copy(q_buf.at[:, win], q_hbm.at[:, win], q_sem.at[i]))
        copies[-1].start()
        start += size
        if i == 0:
            row = lax.broadcasted_iota(jnp.int32, (N, N), 0)
            col = lax.broadcasted_iota(jnp.int32, (N, N), 1)
            r_buf[...] = jnp.where(col >= row, _dot(f_ref[:, :N], f_ref[:, N:LANES], NN, HI), 0.0)
            c_buf[...] = _dot(bta_ref[:, :N], inv_t, NT, HI)[RHS:]
            copies.append(pltpu.make_async_copy(r_buf, r_hbm, small_sem.at[0]))
            copies.append(pltpu.make_async_copy(c_buf, c_hbm, small_sem.at[1]))
            copies[-2].start()
            copies[-1].start()
    for copy in copies:
        copy.wait()


def solution(mesh):
    def local_fn(a_blk, b_blk):
        a_t, b_t = a_blk.T, b_blk.T
        rows = a_t.shape[1]
        factors, bta, a_vmem = pl.pallas_call(
            _reduce_kernel,
            out_shape=[pltpu.VMEM((N, 2 * LANES), F32), pltpu.VMEM((BLK, LANES), F32), pltpu.VMEM((N, rows), F32)],
            in_specs=[pl.BlockSpec(memory_space=pltpu.HBM)] * 2,
            out_specs=[pl.BlockSpec(memory_space=pltpu.VMEM)] * 3,
            scratch_shapes=[
                pltpu.VMEM((RHS, rows), F32),
                pltpu.VMEM((CHIPS, MSG, LANES), F32),
                pltpu.VMEM((2, MSG, LANES), F32),
                pltpu.SemaphoreType.DMA((len(PIECES),)),
                pltpu.SemaphoreType.DMA,
                pltpu.SemaphoreType.DMA((CHIPS - 1,)),
                pltpu.SemaphoreType.DMA((CHIPS - 1,)),
                pltpu.SemaphoreType.DMA((2,)),
            ],
            compiler_params=pltpu.CompilerParams(collective_id=0, has_side_effects=True, vmem_limit_bytes=62_700_000),
        )(a_t, b_t)
        q_t, r, c_t = pl.pallas_call(
            _apply_kernel,
            out_shape=[jax.ShapeDtypeStruct((N, rows), F32), jax.ShapeDtypeStruct((N, N), F32), jax.ShapeDtypeStruct((RHS, N), F32)],
            in_specs=[pl.BlockSpec(memory_space=pltpu.VMEM)] * 3,
            out_specs=[pl.BlockSpec(memory_space=pltpu.HBM)] * 3,
            scratch_shapes=[
                pltpu.VMEM((N, rows), F32),
                pltpu.VMEM((N, N), F32),
                pltpu.VMEM((RHS, N), F32),
                pltpu.SemaphoreType.DMA((len(STORES),)),
                pltpu.SemaphoreType.DMA((2,)),
            ],
            compiler_params=pltpu.CompilerParams(vmem_limit_bytes=48 * 2 ** 20),
        )(factors, bta, a_vmem)
        return q_t.T, r, c_t.T

    return jax.shard_map(local_fn, mesh=mesh, in_specs=(P('rows', None), P('rows', None)), out_specs=(P('rows', None), P(), P()), check_vma=False)
```

```python
import jax
import jax.numpy as jnp
from jax import lax
from jax.experimental import pallas as pl
from jax.experimental.pallas import tpu as pltpu
from jax.sharding import PartitionSpec as P


HI = lax.Precision.HIGHEST
F32 = jnp.float32
N = 64
RHS = 4
BLK = 8
LANES = 128
CHIPS = 8
PIECES = (2048, 4096, 5120, 5120)
SUB = 1024
AHEAD = 3
STORES = (2048,) * 7 + (1024,) * 2
HALF = N // 2
MSG = HALF + BLK
FAR_FIRST = (7, 6, 5, 3, 4, 2, 1)
NT, NN, TN = ((1,), (1,)), ((1,), (0,)), ((0,), (0,))
MESH = pl.DeviceIdType.MESH


def _dot(x, y, dims, precision=None):
    return lax.dot_general(x, y, (dims, ((), ())), precision=precision, preferred_element_type=F32)


def _two_sum(a, b):
    s = a + b
    t = s - a
    return s, (a - (s - t)) + (b - t)


def _scale(x, axis):
    q = jnp.max(jnp.abs(x), axis=axis, keepdims=True) * 8388609.0
    return jnp.abs(q - q * (1.0 - 2.0 ** -24))


def _slices(x, p):
    s1, s2, s3 = p * (1.5 * 2.0 ** 16), p * (1.5 * 2.0 ** 8), p * 1.5
    h1 = (x + s1) - s1
    r1 = x - h1
    h2 = (r1 + s2) - s2
    r2 = r1 - h2
    h3 = (r2 + s3) - s3
    return h1, h2, h3, r2 - h3


def _split3(x):
    c = x * 65537.0
    h1 = c - (c - x)
    r = x - h1
    c = r * 65537.0
    h2 = c - (c - r)
    return h1, h2, r - h2


def _gram_chunk(x, b, px, acc):
    s1, e1, g2, g3, ga, gb = acc
    for q in range(x.shape[1] // SUB):
        h1, h2, h3, l = _slices(x[:, q * SUB:(q + 1) * SUB], px)
        c1, c2, c3 = _split3(b[:, q * SUB:(q + 1) * SUB])
        o = _dot(jnp.concatenate([h1, h2, h3, l], axis=0), jnp.concatenate([h1, h2, h3 + l, c1, c2, c3], axis=0), NT)
        s1, err = _two_sum(s1, o[:N, :2 * N])
        e1 = e1 + err
        g2 = g2 + o[N:2 * N, :2 * N]
        g3 = g3 + (o[2 * N:3 * N, :2 * N] + o[3 * N:, :2 * N])
        ga = ga + (o[:N, 2 * N:] + o[N:2 * N, 2 * N:])
        gb = gb + (o[2 * N:3 * N, 2 * N:] + o[3 * N:, 2 * N:])
    return s1, e1, g2, g3, ga, gb


def _gram_finish(acc):
    s1, e1, g2, g3, ga, gb = acc
    cross = s1[:, N:]
    small = e1[:, N:] + (g3[:, :N] + g3[:, N:])
    z, ez = _two_sum(cross, cross.T)
    h, ea = _two_sum(s1[:, :N], z)
    h, eb = _two_sum(h, g2[:, N:])
    lo = ((ea + eb) + ez) + e1[:, :N] + (small + small.T) + gb[:, :N]
    hi, lo = _two_sum(h, lo)
    ct = (ga + gb)[:, N:].T
    ct = ct[:RHS] + (ct[RHS:2 * RHS] + ct[2 * RHS:])
    return hi, lo, ct


def _pack(hi, lo, bta):
    both = jnp.concatenate([hi, lo], axis=1)
    row = lax.broadcasted_iota(jnp.int32, (HALF, LANES), 0)
    col = lax.broadcasted_iota(jnp.int32, (HALF, LANES), 1) % N
    block = jnp.where(col - HALF > row, jnp.roll(both[:HALF], HALF, axis=1), both[HALF:])
    diag = jnp.sum(jnp.where(row == col, both[:HALF], 0.0), axis=0, keepdims=True)
    sub = lax.broadcasted_iota(jnp.int32, (BLK, LANES), 0)
    tail = jnp.concatenate([jnp.zeros((RHS, LANES), F32), jnp.concatenate([bta, jnp.zeros_like(bta)], axis=1)], axis=0)
    return jnp.concatenate([block, jnp.where(sub == 0, diag, tail)], axis=0)


def _unpack(block, diag):
    row = lax.broadcasted_iota(jnp.int32, (HALF, HALF), 0)
    col = lax.broadcasted_iota(jnp.int32, (HALF, HALF), 1)
    cross, tri = block[:, :HALF], block[:, HALF:]
    flip = tri.T
    first = jnp.where(row == col, diag[:, :HALF], jnp.where(col > row, tri, flip))
    last = jnp.where(col <= row, tri, flip)
    return jnp.concatenate([jnp.concatenate([first, cross.T], axis=1), jnp.concatenate([cross, last], axis=1)], axis=0)


def _fold(both, err):
    lane = lax.broadcasted_iota(jnp.int32, both.shape, 1)
    sub = lax.broadcasted_iota(jnp.int32, both.shape, 0)
    return both + jnp.where((lane >= N) & (sub <= HALF), jnp.roll(err, N, axis=1), 0.0)


def _row(v, k):
    return jnp.broadcast_to(v[k:k + 1, :], (BLK, LANES))


def _factor(g):
    row = lax.broadcasted_iota(jnp.int32, (N, N), 0)
    col = lax.broadcasted_iota(jnp.int32, (N, N), 1)
    full = jnp.concatenate([g, jnp.where(row == col, 1.0, 0.0)], axis=1)
    blocks = N // BLK
    w = [full[BLK * i:BLK * i + BLK] for i in range(blocks)]
    sub = lax.broadcasted_iota(jnp.int32, (BLK, LANES), 0)
    spread = lambda blk, p: [jnp.broadcast_to(blk[:, BLK * p + j:BLK * p + j + 1], (BLK, LANES)) for j in range(BLK)]
    diag = spread(w[0], 0)
    pivot = _row(diag[0], 0)
    out = []
    for p in range(blocks):
        below = [spread(blk, p) for blk in w[p + 1:]]
        ahead = spread(w[p + 1], p + 1) if p + 1 < blocks else None
        cur, pivots_done = w[p], pivot
        for k in range(BLK):
            inv = 1.0 / pivot
            if k > 0:
                pivots_done = jnp.where(sub == k, pivot, pivots_done)
            if k + 1 < BLK:
                link, pivot = _row(diag[k], k + 1), _row(diag[k + 1], k + 1)
                pivot = pivot - (link * link) * inv
            elif ahead is not None:
                link, pivot = _row(below[0][k], 0), _row(ahead[0], 0)
                pivot = pivot - (link * link) * inv
            tops = [_row(diag[j], k) for j in range(k + 1, BLK)]
            mult = jnp.where(sub > k, diag[k], 0.0) * inv
            urow = _row(cur, k)
            for j in range(k + 1, BLK):
                diag[j] = diag[j] - mult * tops[j - k - 1]
            cur = cur - mult * urow
            for i, cols in enumerate(below):
                scaled = cols[k] * inv
                for j in range(k + 1, BLK):
                    cols[j] = cols[j] - scaled * tops[j - k - 1]
                w[p + 1 + i] = w[p + 1 + i] - scaled * urow
                if i == 0:
                    ahead = [ahead[j] - scaled * _row(cols[k], j) for j in range(BLK)]
        out.append(cur * lax.rsqrt(pivots_done))
        diag = ahead
    out = jnp.concatenate(out, axis=0)
    return jnp.where(col >= row, out[:, :N], 0.0), jnp.where(col <= row, out[:, N:], 0.0)


def _exact_rest(first, o1, o2, o3, o4):
    blk = lambda o, i: o[N * i:N * i + N]
    t, e = _two_sum(first, -blk(o1, 0))
    t, ea = _two_sum(t, -blk(o1, 1))
    t, eb = _two_sum(t, -blk(o2, 0))
    t, ec = _two_sum(t, -blk(o2, 1))
    rest = (blk(o1, 2) + blk(o3, 0)) + (blk(o1, 3) + blk(o4, 0)) + ((blk(o2, 2) + blk(o3, 1)) + (blk(o2, 3) + blk(o4, 1)))
    rest = rest + ((blk(o3, 2) + blk(o4, 3)) + (blk(o3, 3) + blk(o4, 2)))
    return (t - rest) + ((e + ea) + (eb + ec))


def _refined(hi, lo):
    row = lax.broadcasted_iota(jnp.int32, (N, N), 0)
    col = lax.broadcasted_iota(jnp.int32, (N, N), 1)
    eye = jnp.where(row == col, 1.0, 0.0)
    r1, v = _factor(jnp.where(row == col, hi * (1.0 + 2.0 ** -19), hi))
    parts = _slices(r1, _scale(r1, 0))
    left = jnp.concatenate(parts, axis=1)
    f = _exact_rest(hi, *[_dot(left, part, TN) for part in parts]) + lo
    left = jnp.concatenate(_slices(v, _scale(v, 1)), axis=0)
    d = _exact_rest(eye, *[_dot(left, part, NT) for part in _slices(r1, _scale(r1, 1))])
    d = jnp.where(col <= row, d, 0.0)
    e = _dot(_dot(v, f, NN, HI), v, NT, HI) + (_dot(d, d, NT, HI) - (d + d.T))
    r2, v2 = _factor(eye + e)
    return r2, r1 + _dot(d, r1, TN, HI), v2, v


def _reduce_kernel(a_hbm, b_hbm, f_ref, bta_ref, a_buf, b_buf, slots, sums, a_sem, b_sem, send_sem, recv_sem, down_sem):
    me = lax.axis_index('rows')
    core = me % 2
    chip = me // 2
    partner = me + 1 - 2 * core
    steps = len(PIECES)
    edges = [sum(PIECES[:i]) for i in range(steps + 1)]
    copies = []
    for i in range(steps):
        win = pl.ds(edges[i], PIECES[i])
        copies.append(pltpu.make_async_copy(a_hbm.at[:, win], a_buf.at[:, win], a_sem.at[i]))
    b_copy = pltpu.make_async_copy(b_hbm, b_buf, b_sem)
    for copy in copies[:1] + [b_copy] + copies[1:AHEAD]:
        copy.start()
    barrier = pltpu.get_barrier_semaphore()
    x, y, z = chip % 2, (chip // 2) % 2, chip // 4
    flip = lambda bit, way: 1 - bit if way else bit
    peers = [8 * flip(z, far // 4) + 4 * flip(y, far // 2 % 2) + 2 * flip(x, far % 2) + core for far in FAR_FIRST]
    for peer in peers + [partner]:
        pl.semaphore_signal(barrier, inc=1, device_id=(peer,), device_id_type=MESH)

    zero = jnp.zeros((N, 2 * N), F32)
    wide = jnp.zeros((N, N + 3 * RHS), F32)
    acc = (zero, zero, zero, zero, wide, wide)
    scale = None
    for i in range(steps + 1):
        nxt = None
        if i < steps:
            copies[i].wait()
            if i + AHEAD < steps:
                copies[i + AHEAD].start()
            nxt = _scale(a_buf[:, edges[i]:edges[i + 1]], 1)
        if i == 0:
            b_copy.wait()
        if i > 0:
            win = slice(edges[i - 1], edges[i])
            acc = _gram_chunk(a_buf[:, win], b_buf[:, win], scale, acc)
        scale = nxt
    hi, lo, bta = _gram_finish(acc)
    slots[pl.ds(chip, 1)] = _pack(hi, lo, bta)[None]
    pl.semaphore_wait(barrier, CHIPS)
    sends = [pltpu.make_async_remote_copy(
        src_ref=slots.at[chip], dst_ref=slots.at[chip], send_sem=send_sem.at[j], recv_sem=recv_sem.at[j],
        device_id=(peer,), device_id_type=MESH) for j, peer in enumerate(peers)]
    for send in sends:
        send.start()
    for send in sends:
        send.wait_recv()
    both, err = slots[0], jnp.zeros((MSG, LANES), F32)
    for j in range(1, CHIPS):
        both, e = _two_sum(both, slots[j])
        err = err + e
    sums[pl.ds(core, 1)] = _fold(both, err)[None]
    swap = pltpu.make_async_remote_copy(
        src_ref=sums.at[core], dst_ref=sums.at[core], send_sem=down_sem.at[0], recv_sem=down_sem.at[1],
        device_id=(partner,), device_id_type=MESH)
    swap.start()
    swap.wait_recv()
    got = _fold(*_two_sum(sums[0], sums[1]))
    r2, rc, v2, v = _refined(*[_unpack(got[:HALF, side:side + N], got[HALF:HALF + 1, side:side + N]) for side in (0, N)])
    f_ref[:, :LANES] = jnp.concatenate([r2, rc], axis=1)
    f_ref[:, LANES:] = jnp.concatenate([v2, v], axis=1)
    bta_ref[...] = got[HALF:, :]
    for send in sends:
        send.wait_send()
    swap.wait_send()


def _apply_kernel(f_ref, bta_ref, a_ref, q_hbm, r_hbm, c_hbm, q_buf, r_buf, c_buf, q_sem, small_sem):
    inv_t = _dot(f_ref[:, LANES:LANES + N], f_ref[:, LANES + N:], NN, HI)
    w = jnp.concatenate([jnp.concatenate([m] * 3, axis=1) for m in _split3(inv_t)], axis=0)
    copies = []
    start = 0
    for i, size in enumerate(STORES):
        win = pl.ds(start, size)
        o = _dot(w, jnp.concatenate(_split3(a_ref[:, win]), axis=0), NN)
        q_buf[:, win] = o[:N] + (o[N:2 * N] + o[2 * N:])
        copies.append(pltpu.make_async_copy(q_buf.at[:, win], q_hbm.at[:, win], q_sem.at[i]))
        copies[-1].start()
        start += size
        if i == 0:
            row = lax.broadcasted_iota(jnp.int32, (N, N), 0)
            col = lax.broadcasted_iota(jnp.int32, (N, N), 1)
            r_buf[...] = jnp.where(col >= row, _dot(f_ref[:, :N], f_ref[:, N:LANES], NN, HI), 0.0)
            c_buf[...] = _dot(bta_ref[:, :N], inv_t, NT, HI)[RHS:]
            copies.append(pltpu.make_async_copy(r_buf, r_hbm, small_sem.at[0]))
            copies.append(pltpu.make_async_copy(c_buf, c_hbm, small_sem.at[1]))
            copies[-2].start()
            copies[-1].start()
    for copy in copies:
        copy.wait()


def solution(mesh):
    def local_fn(a_blk, b_blk):
        a_t, b_t = a_blk.T, b_blk.T
        rows = a_t.shape[1]
        factors, bta, a_vmem = pl.pallas_call(
            _reduce_kernel,
            out_shape=[pltpu.VMEM((N, 2 * LANES), F32), pltpu.VMEM((BLK, LANES), F32), pltpu.VMEM((N, rows), F32)],
            in_specs=[pl.BlockSpec(memory_space=pltpu.HBM)] * 2,
            out_specs=[pl.BlockSpec(memory_space=pltpu.VMEM)] * 3,
            scratch_shapes=[
                pltpu.VMEM((RHS, rows), F32),
                pltpu.VMEM((CHIPS, MSG, LANES), F32),
                pltpu.VMEM((2, MSG, LANES), F32),
                pltpu.SemaphoreType.DMA((len(PIECES),)),
                pltpu.SemaphoreType.DMA,
                pltpu.SemaphoreType.DMA((CHIPS - 1,)),
                pltpu.SemaphoreType.DMA((CHIPS - 1,)),
                pltpu.SemaphoreType.DMA((2,)),
            ],
            compiler_params=pltpu.CompilerParams(collective_id=0, has_side_effects=True, vmem_limit_bytes=62_700_000),
        )(a_t, b_t)
        q_t, r, c_t = pl.pallas_call(
            _apply_kernel,
            out_shape=[jax.ShapeDtypeStruct((N, rows), F32), jax.ShapeDtypeStruct((N, N), F32), jax.ShapeDtypeStruct((RHS, N), F32)],
            in_specs=[pl.BlockSpec(memory_space=pltpu.VMEM)] * 3,
            out_specs=[pl.BlockSpec(memory_space=pltpu.HBM)] * 3,
            scratch_shapes=[
                pltpu.VMEM((N, rows), F32),
                pltpu.VMEM((N, N), F32),
                pltpu.VMEM((RHS, N), F32),
                pltpu.SemaphoreType.DMA((len(STORES),)),
                pltpu.SemaphoreType.DMA((2,)),
            ],
            compiler_params=pltpu.CompilerParams(vmem_limit_bytes=48 * 2 ** 20),
        )(factors, bta, a_vmem)
        return q_t.T, r, c_t.T

    return jax.shard_map(local_fn, mesh=mesh, in_specs=(P('rows', None), P('rows', None)), out_specs=(P('rows', None), P(), P()), check_vma=False)
```
